32 devices in a mesh: rep: 4 (over x, y), dp: 8 (over z, core).
Axes of the slice: x: 2, y: 2, z: 4, core: 2. Of those that a mesh axis runs over, the one named last changes fastest.
Arguments:
- g_w_gate: bfloat16 [32, 2, 1024, 3328], P(('rep', 'dp')), parts along dimension 0
- g_w_up: bfloat16 [32, 2, 1024, 3328], P(('rep', 'dp')), parts along dimension 0
- g_w_down: bfloat16 [32, 2, 3328, 1024], P(('rep', 'dp')), parts along dimension 0
- w_gate: bfloat16 [2, 1024, 3328], replicated
- w_up: bfloat16 [2, 1024, 3328], replicated
- w_down: bfloat16 [2, 3328, 1024], replicated
- m_w_gate: float32 [2, 1024, 3328], P(None, 'dp')
- m_w_up: float32 [2, 1024, 3328], P(None, 'dp')
- m_w_down: float32 [2, 3328, 1024], P(None, 'dp')
- v_w_gate: float32 [2, 1024, 3328], P(None, 'dp')
- v_w_up: float32 [2, 1024, 3328], P(None, 'dp')
- v_w_down: float32 [2, 3328, 1024], P(None, 'dp')
Outputs:
- output 1: bfloat16 [8, 1024, 3328], P('rep'), parts along dimension 0
- output 2: bfloat16 [8, 1024, 3328], P('rep'), parts along dimension 0
- output 3: bfloat16 [8, 3328, 1024], P('rep'), parts along dimension 0
- output 4: float32 [8, 1024, 3328], P('rep', 'dp'), parts along dimension 0
- output 5: float32 [8, 1024, 3328], P('rep', 'dp'), parts along dimension 0
- output 6: float32 [8, 3328, 1024], P('rep', 'dp'), parts along dimension 0
- output 7: float32 [8, 1024, 3328], P('rep', 'dp'), parts along dimension 0
- output 8: float32 [8, 1024, 3328], P('rep', 'dp'), parts along dimension 0
- output 9: float32 [8, 3328, 1024], P('rep', 'dp'), parts along dimension 0
There are 4 independent parts. The reference program is written for one: setup_inputs(seed, part) draws one part's arguments, and reference() takes and returns one part's arrays. A program takes and returns all parts, laid end to end along the dimension named above; an argument that names none is the same for every part.
All inputs are finite; a program needn't handle non-finite values.
Results may differ from the reference program's by a relative error of at most 0.022.
Values are sent between devices in bfloat16 or wider.
A program may use at most 2 GiB of HBM per device.

```python
import jax
import jax.numpy as jnp
from jax import lax

DEVICES = 8
D = 1024
FF = 3328
LAYERS = 2
NAMES = ("w_gate", "w_up", "w_down")
SHAPES = {"w_gate": (LAYERS, D, FF), "w_up": (LAYERS, D, FF), "w_down": (LAYERS, FF, D)}


def setup_inputs(seed: int = 0, part: int = 0) -> dict:
    kz, *keys = jax.random.split(jax.random.key(seed), 1 + 5 * len(NAMES))
    loud = 2.0 ** jax.random.uniform(kz, (), jnp.float32, -1.0, 1.0)
    drawn = {}
    for name, key, both in zip(NAMES, keys[:3], keys[3:6], strict=True):
        own = jax.random.normal(jax.random.fold_in(key, part), (DEVICES, *SHAPES[name]), jnp.float32)
        shared = jax.random.normal(jax.random.fold_in(both, part), SHAPES[name], jnp.float32)
        drawn["g_" + name] = (loud * (0.7 * shared / DEVICES + 0.7 * own * DEVICES**-0.5)).astype(jnp.bfloat16)
    for name, key in zip(NAMES, keys[6:9], strict=True):
        drawn[name] = (jax.random.normal(key, SHAPES[name], jnp.float32) * SHAPES[name][1] ** -0.5).astype(jnp.bfloat16)
    for name, key in zip(NAMES, keys[9:12], strict=True):
        drawn["m_" + name] = loud * 0.5 * jax.random.normal(key, SHAPES[name], jnp.float32)
    for name, key in zip(NAMES, keys[12:15], strict=True):
        drawn["v_" + name] = loud * loud * jax.random.uniform(key, SHAPES[name], jnp.float32, 0.5, 1.5)
    return drawn


def adamw(w, m, v, g):
    m = 0.9 * m + 0.1 * g
    v = 0.95 * v + 0.05 * g * g
    step = m * lax.rsqrt(v + 1e-8) + 0.1 * w
    return (w - 0.02 * step).astype(jnp.bfloat16), m, v


def clipped(gradients, sum_of_squares, count):
    factor = jnp.minimum(1.0, 0.5 * lax.rsqrt(sum_of_squares / count + 1e-30))
    return [g * factor for g in gradients]


def reference(g_w_gate, g_w_up, g_w_down, w_gate, w_up, w_down, m_w_gate, m_w_up, m_w_down, v_w_gate, v_w_up, v_w_down):
    def total(terms):
        return lax.scan(lambda so_far, term: (so_far + term.astype(jnp.float32), None), jnp.zeros(terms.shape[1:], jnp.float32), terms)[0]

    gradients = [total(terms).astype(jnp.bfloat16).astype(jnp.float32) for terms in (g_w_gate, g_w_up, g_w_down)]
    gradients = clipped(gradients, sum(jnp.sum(g * g) for g in gradients), sum(g.size for g in gradients))
    new = [
        adamw(w.astype(jnp.float32), m, v, g)
        for w, m, v, g in zip((w_gate, w_up, w_down), (m_w_gate, m_w_up, m_w_down), (v_w_gate, v_w_up, v_w_down), gradients, strict=True)
    ]
    return tuple(one[which] for which in range(3) for one in new)
```

```python
import functools

import jax
import jax.numpy as jnp
from jax import lax
from jax.experimental import pallas as pl
from jax.experimental.pallas import tpu as pltpu
from jax.sharding import PartitionSpec as P

F32, BF16 = jnp.float32, jnp.bfloat16
HALVES = 2
CHUNKS = 4
GROUP = 8
ROWS = 16


def kernel(count, *refs):
    g, w, m, v = refs[0:3], refs[3:6], refs[6:9], refs[9:12]
    t, gout, fout = refs[12:15], refs[15:18], refs[18]
    x, ein, iin = refs[19:22], refs[22:25], refs[25:28]
    inb, outr, outl = refs[28:30], refs[30:32], refs[32:34]
    mb, vb, wb = refs[34:36], refs[36:38], refs[38:40]
    gv, wn = refs[40:43], refs[43:46]
    nb, fbuf = refs[46:48]
    (ld, osr, osl, xs, xr, er, ir, up, ns, nr, ar, pr, so, si, sp, sl, gs) = refs[48:]

    me = lax.axis_index("dp")
    z, k = me // 2, me % 2
    h = z // 2
    is_end = (z % 3) == 0
    inner, outer = 2 * (z + 1 - 2 * h) + k, 2 * (z - 1 + 2 * h) + k
    partner = 2 * z + 1 - k
    kind = (0, 0, 1)
    rows_of = [r.shape[1] for r in m]
    half_of = [r // HALVES for r in rows_of]

    def chip(J):
        return J + h * (3 - 2 * J)

    def at_layer(q):
        return q // HALVES, q % HALVES

    def full(ref, a, J, parity, q):
        l, s = at_layer(q)
        start = pl.multiple_of((2 * chip(J) + parity) * rows_of[a] + s * half_of[a], 16)
        return ref.at[l, pl.ds(start, half_of[a]), :]

    def part(ref, a, q):
        l, s = at_layer(q)
        return ref.at[l, pl.ds(pl.multiple_of(s * half_of[a], 16), half_of[a]), :]

    def remote(src, dst, send, recv, to):
        return pltpu.make_async_remote_copy(src, dst, send, recv, device_id={"dp": to}, device_id_type=pl.DeviceIdType.MESH)

    barrier = pltpu.get_barrier_semaphore()
    for d in range(1, GROUP):
        pl.semaphore_signal(barrier, inc=1, device_id={"dp": (me + d) % GROUP}, device_id_type=pl.DeviceIdType.MESH)
    pl.semaphore_wait(barrier, GROUP - 1)

    def swap(J, a, l):
        start = pl.multiple_of((2 * chip(J) + 1 - k) * rows_of[a], 16)
        return remote(g[a].at[0, l, pl.ds(start, rows_of[a]), :], x[a].at[J, l], xs.at[J * 6 + a * 2 + l], xr.at[J * 6 + a * 2 + l], partner)

    for J in (3, 0, 2, 1):
        for a in range(3):
            for l in range(2):
                swap(J, a, l).start()

    def moments(a, q):
        slot, c = q % 2, kind[a]
        return (
            pltpu.make_async_copy(part(m[a], a, q), mb[c].at[slot], up.at[slot]),
            pltpu.make_async_copy(part(v[a], a, q), vb[c].at[slot], up.at[2 + slot]),
            pltpu.make_async_copy(full(w[a], a, 0 * q + own_J, k, q), wb[c].at[slot], up.at[4 + slot]),
        )

    own_J = jnp.where(is_end, 0, 1)
    for copy in moments(0, 0):
        copy.start()

    def load(a, J, q, more):
        l, s = at_layer(q)

        @pl.when(s == 0)
        def _():
            remote(x[a].at[J, l], x[a].at[J, l], xs.at[J * 6 + a * 2 + l], xr.at[J * 6 + a * 2 + l], partner).wait_recv()

        sources = [full(g[a].at[0], a, J, k, q), part(x[a].at[J], a, q), *more]
        copies = [pltpu.make_async_copy(src, inb[kind[a]].at[i], ld.at[i]) for i, src in enumerate(sources)]
        for copy in copies:
            copy.start()
        for copy in copies:
            copy.wait()
        return len(copies)

    def total(a, n, r):
        here = pl.ds(pl.multiple_of(r * ROWS, ROWS), ROWS)
        so_far = inb[kind[a]][0, here, :].astype(F32)
        for i in range(1, n):
            so_far = so_far + inb[kind[a]][i, here, :].astype(F32)
        return so_far.astype(BF16)

    def send(a, J, q, more, out, sem, dst, recv, to, first):
        c = kind[a]
        copy = remote(out[c].at[q], dst, sem.at[c * CHUNKS + q], recv, to)
        n = load(a, J, q, more)
        if not first:
            copy.wait_send()

        def row(r, _):
            out[c][q, pl.ds(pl.multiple_of(r * ROWS, ROWS), ROWS), :] = total(a, n, r)
            return 0

        lax.fori_loop(0, half_of[a] // ROWS, row, 0)
        copy.start()

    def final(a, J, q, more, acc):
        l, s = at_layer(q)
        n = load(a, J, q, more)

        def row(r, acc):
            one = total(a, n, r)
            gv[a][l, pl.ds(pl.multiple_of(s * half_of[a] + r * ROWS, ROWS), ROWS), :] = one
            one = one.astype(F32)
            one = one * one
            for i in range(one.shape[1] // 128):
                acc = acc + one[:, i * 128 : (i + 1) * 128]
            return acc

        return lax.fori_loop(0, half_of[a] // ROWS, row, acc)

    def from_end(a, p, q):
        i = p * 12 + a * CHUNKS + q
        return remote(part(ein[a].at[p], a, q), part(ein[a].at[p], a, q), osr.at[0], er.at[i], outer)

    def from_inner(a, p, q):
        i = p * 12 + a * CHUNKS + q
        return remote(part(iin[a].at[p], a, q), part(iin[a].at[p], a, q), osr.at[0], ir.at[i], inner)

    def loop(body):
        lax.fori_loop(0, CHUNKS, lambda q, _: (body(q), 0)[1], 0)

    zero = jnp.zeros((ROWS, 128), F32)

    def drain(out, sem):
        for a in (1, 2):
            for q in range(CHUNKS):
                remote(out[kind[a]].at[q], out[kind[a]].at[q], sem.at[kind[a] * CHUNKS + q], sem.at[kind[a] * CHUNKS + q], inner).wait_send()

    @pl.when(is_end)
    def _():
        acc = zero
        for p in range(3):
            for a in range(3):

                def both(q, acc, p=p, a=a):
                    i = p * 12 + a * CHUNKS + q
                    send(a, 3 - p, q, [], outr, osr, part(ein[a].at[p], a, q), er.at[i], inner, p == 0 and a != 1)
                    if p == 1:
                        from_inner(a, 0, q).wait_recv()
                        acc = final(a, 0, q, [part(iin[a].at[0], a, q)], acc)
                    return acc

                acc = lax.fori_loop(0, CHUNKS, both, acc)
        fbuf[...] = acc[:8] + acc[8:]
        drain(outr, osr)

    @pl.when(jnp.logical_not(is_end))
    def _():
        def inward(p, a, q):
            from_end(a, p, q).wait_recv()
            i = p * 12 + a * CHUNKS + q
            send(a, 3 - p, q, [part(ein[a].at[p], a, q)], outr, osr, part(iin[a].at[p], a, q), ir.at[i], inner, p == 0 and a != 1)

        def outward(a, q):
            from_inner(a, 0, q).wait_recv()
            send(a, 0, q, [part(iin[a].at[0], a, q)], outl, osl, part(iin[a].at[0], a, q), ir.at[a * CHUNKS + q], outer, a != 1)

        for a in range(4):

            def both(q, a=a):
                if a < 3:
                    inward(0, a, q)
                if a > 0:
                    outward(a - 1, q)

            loop(both)
        for a in range(3):
            loop(functools.partial(inward, 1, a))
        acc = zero
        for a in range(3):

            def last(q, acc, a=a):
                from_inner(a, 1, q).wait_recv()
                from_end(a, 2, q).wait_recv()
                return final(a, 1, q, [part(ein[a].at[2], a, q), part(iin[a].at[1], a, q)], acc)

            acc = lax.fori_loop(0, CHUNKS, last, acc)
        fbuf[...] = acc[:8] + acc[8:]
        drain(outr, osr)
        drain(outl, osl)

    nb[me] = fbuf[...]
    sums = [remote(nb.at[me], nb.at[me], ns.at[d], nr.at[d], (me + d) % GROUP) for d in range(1, GROUP)]
    for copy in sums:
        copy.start()
    for a in range(3):
        pltpu.make_async_copy(gv[a], gout[a], gs.at[a]).start()
    for copy in sums:
        copy.wait()
    squares = nb[0]
    for d in range(1, GROUP):
        squares = squares + nb[d]
    squares = jnp.sum(jnp.sum(squares, axis=0, keepdims=True), axis=1, keepdims=True)
    factor = jnp.minimum(1.0, 0.5 * lax.rsqrt(squares / count + 1e-30))
    fbuf[...] = jnp.broadcast_to(factor, fbuf.shape)
    fout[...] = fbuf[...]

    def give(a, q, J, src, to_inner, to_outer):
        c = a * CHUNKS + q
        dst = full(t[a], a, J, k, q)
        remote(src, dst, sp.at[J * 12 + c], pr.at[J * 12 + c], partner).start()
        if to_inner is not None:
            remote(src, dst, si.at[to_inner[0] * 12 + c], ar.at[to_inner[1] * 12 + c], inner).start()
        if to_outer is not None:
            remote(src, dst, so.at[to_outer * 12 + c], ar.at[to_outer * 12 + c], outer).start()

    for a in range(3):

        def update(q, a=a):
            c, slot = kind[a], q % 2
            l, s = at_layer(q)
            for copy in moments(a, q):
                copy.wait()

            @pl.when(q < CHUNKS - 1)
            def _():
                for copy in moments(a, q + 1):
                    copy.start()

            if a < 2:

                @pl.when(q == CHUNKS - 1)
                def _():
                    for copy in moments(a + 1, q * 0):
                        copy.start()

            def row(r, _):
                here = pl.ds(pl.multiple_of(r * ROWS, ROWS), ROWS)
                there = pl.ds(pl.multiple_of(s * half_of[a] + r * ROWS, ROWS), ROWS)
                one = gv[a][l, there, :].astype(F32) * fbuf[0:1, 0:1]
                m1 = 0.9 * mb[c][slot, here, :] + 0.1 * one
                v1 = 0.95 * vb[c][slot, here, :] + 0.05 * one * one
                old = wb[c][slot, here, :].astype(F32)
                wn[a][l, there, :] = (old - 0.02 * (m1 * lax.rsqrt(v1 + 1e-8) + 0.1 * old)).astype(BF16)
                return 0

            lax.fori_loop(0, half_of[a] // ROWS, row, 0)
            src = part(wn[a], a, q)

            @pl.when(is_end)
            def _():
                give(a, q, 0, src, (0, 2), None)

            @pl.when(jnp.logical_not(is_end))
            def _():
                give(a, q, 1, src, (0, 0), 0)

            pltpu.make_async_copy(src, full(t[a], a, own_J, k, q), sl.at[a * CHUNKS + q]).start()

        loop(update)

    def arrived(a, q, J, slot):
        here = full(t[a], a, J, k, q)
        remote(here, here, sl.at[0], ar.at[slot * 12 + a * CHUNKS + q], inner).wait_recv()

    @pl.when(is_end)
    def _():
        for slot in range(3):
            for a in range(3):

                def on(q, a=a, slot=slot):
                    arrived(a, q, slot + 1, slot)
                    give(a, q, slot + 1, full(t[a], a, slot + 1, k, q), None, None)

                loop(on)

    @pl.when(jnp.logical_not(is_end))
    def _():
        for a in range(3):

            def on(q, a=a):
                arrived(a, q, 2, 0)
                give(a, q, 2, full(t[a], a, 2, k, q), None, 1)
                arrived(a, q, 0, 2)
                give(a, q, 0, full(t[a], a, 0, k, q), (1, 1), None)

            loop(on)
        for a in range(3):

            def on(q, a=a):
                arrived(a, q, 3, 1)
                give(a, q, 3, full(t[a], a, 3, k, q), None, 2)

            loop(on)

    for a in range(3):

        def rest(q, a=a):
            c = a * CHUNKS + q
            for J in range(4):
                mine, theirs = full(t[a], a, J, k, q), full(t[a], a, J, 1 - k, q)
                remote(mine, mine, sp.at[J * 12 + c], pr.at[J * 12 + c], partner).wait_send()
                remote(theirs, theirs, sp.at[J * 12 + c], pr.at[J * 12 + c], partner).wait_recv()
            here = full(t[a], a, own_J, k, q)
            pltpu.make_async_copy(part(wn[a], a, q), here, sl.at[c]).wait()
            remote(here, here, si.at[c], ar.at[c], inner).wait_send()

            @pl.when(jnp.logical_not(is_end))
            def _():
                remote(here, here, si.at[12 + c], ar.at[c], inner).wait_send()
                for n in range(3):
                    remote(here, here, so.at[n * 12 + c], ar.at[c], outer).wait_send()

        loop(rest)
        pltpu.make_async_copy(gv[a], gout[a], gs.at[a]).wait()
        for J in range(4):
            for l in range(2):
                swap(J, a, l).wait_send()


def solution(mesh):
    def step(*arrays):
        terms, weights, m, v = (arrays[i : i + 3] for i in (0, 3, 6, 9))
        blocks = [one.shape for one in m]
        count = GROUP * sum(one.size for one in m)
        pair = (blocks[0], blocks[2])
        chunk = [(one[1] // HALVES, one[2]) for one in pair]
        any_space = pl.BlockSpec(memory_space=pl.ANY)
        out_shape = (
            [jax.ShapeDtypeStruct(one.shape, BF16) for one in weights]
            + [jax.ShapeDtypeStruct(one, BF16) for one in blocks]
            + [jax.ShapeDtypeStruct((8, 128), F32)]
            + [jax.ShapeDtypeStruct((4, *one), BF16) for one in blocks]
            + [jax.ShapeDtypeStruct((3, *one), BF16) for one in blocks]
            + [jax.ShapeDtypeStruct((2, *one), BF16) for one in blocks]
        )
        out_specs = [any_space] * 6 + [pl.BlockSpec(memory_space=pltpu.VMEM)] + [any_space] * 9
        dma = pltpu.SemaphoreType.DMA
        scratch = (
            [pltpu.VMEM((4, *one), BF16) for one in chunk]
            + [pltpu.VMEM((CHUNKS, *one), BF16) for one in chunk]
            + [pltpu.VMEM((CHUNKS, *one), BF16) for one in chunk]
            + [pltpu.VMEM((2, *one), F32) for one in chunk]
            + [pltpu.VMEM((2, *one), F32) for one in chunk]
            + [pltpu.VMEM((2, *one), BF16) for one in chunk]
            + [pltpu.VMEM(one, BF16) for one in blocks]
            + [pltpu.VMEM(one, BF16) for one in blocks]
            + [pltpu.VMEM((GROUP, 8, 128), F32), pltpu.VMEM((8, 128), F32)]
            + [dma((n,)) for n in (4, 8, 8, 24, 24, 36, 24, 6, 8, 8, 36, 48, 36, 24, 48, 12, 3)]
        )
        out = pl.pallas_call(
            functools.partial(kernel, count),
            out_shape=out_shape,
            in_specs=[any_space] * 12,
            out_specs=out_specs,
            scratch_shapes=scratch,
            compiler_params=pltpu.CompilerParams(collective_id=0, has_side_effects=True, vmem_limit_bytes=48 * 2**20),
            name="step",
        )(*arrays)
        whole, sums, factor = out[:3], out[3:6], out[6][0, 0]
        new_m, new_v = [], []
        for one, m1, v1 in zip(sums, m, v, strict=True):
            one = one.astype(F32) * factor
            new_m.append(0.9 * m1 + 0.1 * one)
            new_v.append(0.95 * v1 + 0.05 * one * one)
        return (*whole, *new_m, *new_v)

    all_of, cut = P(None, None, None), P(None, "dp", None)
    return jax.shard_map(
        step,
        mesh=mesh,
        in_specs=(P(("rep", "dp"), None, None, None),) * 3 + (all_of,) * 3 + (cut,) * 6,
        out_specs=(P("rep", None, None),) * 3 + (P("rep", "dp", None),) * 6,
        check_vma=False,
    )
```

```python
import functools

import jax
import jax.numpy as jnp
from jax import lax
from jax.experimental import pallas as pl
from jax.experimental.pallas import tpu as pltpu
from jax.sharding import PartitionSpec as P

F32, BF16 = jnp.float32, jnp.bfloat16
HALVES = 2
CHUNKS = 4
GROUP = 8
LENT = 0
ORDER = (1, 2, 0)
OUTR, OUTL = 4, 6
LIMIT = 5 * 2**20
ROWS = 16


def kernel(count, *refs):
    g, w, m, v = refs[0:3], refs[3:6], refs[6:9], refs[9:12]
    t, nm, nv = refs[12:15], refs[15:18], refs[18:21]
    x, ein, iin = refs[21:24], refs[24:27], refs[27:30]
    xm, xv = refs[30:32]
    wb, lm, lv = refs[32:34], refs[34], refs[35]
    nb, fbuf = refs[36:38]
    (ld, osr, osl, xs, xr, er, ir, up, ns, nr, ar, pr, so, si, sp, ms, mr, hs, hr, mo) = refs[38:]

    me = lax.axis_index("dp")
    z, k = me // 2, me % 2
    h = z // 2
    is_end = (z % 3) == 0
    inner, outer = 2 * (z + 1 - 2 * h) + k, 2 * (z - 1 + 2 * h) + k
    partner = 2 * z + 1 - k
    kind = (0, 0, 1)
    rows_of = [r.shape[1] for r in m]
    half_of = [r // HALVES for r in rows_of]

    def chip(J):
        return J + h * (3 - 2 * J)

    def at_layer(q):
        return q // HALVES, q % HALVES

    def full(ref, a, J, parity, q):
        l, s = at_layer(q)
        start = pl.multiple_of((2 * chip(J) + parity) * rows_of[a] + s * half_of[a], 16)
        return ref.at[l, pl.ds(start, half_of[a]), :]

    def part(ref, a, q):
        l, s = at_layer(q)
        return ref.at[l, pl.ds(pl.multiple_of(s * half_of[a], 16), half_of[a]), :]

    def slot_start(c, i):
        rows, half = rows_of[c + 1], half_of[c + 1]
        return pl.multiple_of(((2 * z + k) * rows + rows + i * half) % (GROUP * rows), 16)

    def staged(c, i):
        return t[c + 1].at[0, pl.ds(slot_start(c, i), half_of[c + 1]), :]

    def staged_rows(c, i, r):
        return 0, pl.ds(pl.multiple_of(slot_start(c, i) + r * ROWS, ROWS), ROWS), slice(None)

    def remote(src, dst, send, recv, to):
        return pltpu.make_async_remote_copy(src, dst, send, recv, device_id={"dp": to}, device_id_type=pl.DeviceIdType.MESH)

    barrier = pltpu.get_barrier_semaphore()
    for d in range(1, GROUP):
        pl.semaphore_signal(barrier, inc=1, device_id={"dp": (me + d) % GROUP}, device_id_type=pl.DeviceIdType.MESH)
    pl.semaphore_wait(barrier, GROUP - 1)

    def swap(J, a, l):
        start = pl.multiple_of((2 * chip(J) + 1 - k) * rows_of[a], 16)
        return remote(g[a].at[0, l, pl.ds(start, rows_of[a]), :], x[a].at[J, l], xs.at[J * 6 + a * 2 + l], xr.at[J * 6 + a * 2 + l], partner)

    def give_terms(J, weights=(0, 1, 2)):
        for a in weights:
            for l in range(2):
                swap(J, a, l).start()

    give_terms(3, (0,))

    own_J = jnp.where(is_end, 0, 1)

    def old_weight(a, q, J=own_J):
        return pltpu.make_async_copy(full(w[a], a, J, k, q), wb[kind[a]].at[q % 2], up.at[q % 2])

    old_weight(ORDER[0], 0).start()

    def moments(a):
        return pltpu.make_async_copy(m[a], nm[a], mo.at[a]), pltpu.make_async_copy(v[a], nv[a], mo.at[3 + a])

    def load(a, J, q, more):
        l, s = at_layer(q)

        @pl.when(s == 0)
        def _():
            remote(x[a].at[J, l], x[a].at[J, l], xs.at[J * 6 + a * 2 + l], xr.at[J * 6 + a * 2 + l], partner).wait_recv()

        sources = [full(g[a].at[0], a, J, k, q), part(x[a].at[J], a, q), *more]
        copies = [pltpu.make_async_copy(src, staged(kind[a], i), ld.at[i]) for i, src in enumerate(sources)]
        for copy in copies:
            copy.start()
        for copy in copies:
            copy.wait()
        return len(copies)

    def total(a, n, r):
        so_far = t[kind[a] + 1][staged_rows(kind[a], 0, r)].astype(F32)
        for i in range(1, n):
            so_far = so_far + t[kind[a] + 1][staged_rows(kind[a], i, r)].astype(F32)
        return so_far.astype(BF16)

    def send(a, J, q, more, out, sem, dst, recv, to, first):
        c, slot = kind[a], q % 2
        copy = remote(staged(c, out + slot), dst, sem.at[c * 2 + slot], recv, to)
        n = load(a, J, q, more)
        if first:

            @pl.when(q >= 2)
            def _():
                copy.wait_send()
        else:
            copy.wait_send()

        def row(r, _):
            t[c + 1][staged_rows(c, out + slot, r)] = total(a, n, r)
            return 0

        lax.fori_loop(0, half_of[a] // ROWS, row, 0)
        copy.start()

    def final(a, J, q, more, acc):
        l, s = at_layer(q)
        n = load(a, J, q, more)

        def row(r, acc):
            one = total(a, n, r)
            t[a][l, pl.ds(pl.multiple_of((2 * z + k) * rows_of[a] + s * half_of[a] + r * ROWS, ROWS), ROWS), :] = one
            one = one.astype(F32)
            one = one * one
            for i in range(one.shape[1] // 128):
                acc = acc + one[:, i * 128 : (i + 1) * 128]
            return acc

        return lax.fori_loop(0, half_of[a] // ROWS, row, acc)

    def more_terms(p, a, q):
        if p == 0 and a == 0:

            @pl.when(q == 1)
            def _():
                give_terms(3, (1, 2))

    def from_end(a, p, q):
        i = p * 12 + a * CHUNKS + q
        return remote(part(ein[a].at[p], a, q), part(ein[a].at[p], a, q), osr.at[0], er.at[i], outer)

    def from_inner(a, p, q):
        i = p * 12 + a * CHUNKS + q
        return remote(part(iin[a].at[p], a, q), part(iin[a].at[p], a, q), osr.at[0], ir.at[i], inner)

    def lend(l):
        return (
            remote(m[LENT].at[l], xm.at[l], ms.at[l], mr.at[l], outer),
            remote(v[LENT].at[l], xv.at[l], ms.at[2 + l], mr.at[2 + l], outer),
        )

    def lend_sum(q):
        here = full(t[LENT], LENT, 1, k, q)
        return remote(here, here, hs.at[q], hr.at[q], outer)

    def loop(body):
        lax.fori_loop(0, CHUNKS, lambda q, _: (body(q), 0)[1], 0)

    zero = jnp.zeros((ROWS, 128), F32)

    def drain(out, sem):
        for a in (1, 2):
            for slot in range(2):
                one, on = staged(kind[a], out + slot), sem.at[kind[a] * 2 + slot]
                remote(one, one, on, on, inner).wait_send()

    @pl.when(is_end)
    def _():
        acc = zero
        for p in range(3):
            for a in range(3):

                if p == 0 and a > 0:
                    give_terms((0, 2)[a - 1])
                if p == 1 and a == 0:
                    give_terms(1)
                if p == 1:
                    for copy in moments(a):
                        copy.start()

                def both(q, acc, p=p, a=a):
                    i = p * 12 + a * CHUNKS + q
                    more_terms(p, a, q)
                    send(a, 3 - p, q, [], OUTR, osr, part(ein[a].at[p], a, q), er.at[i], inner, p == 0 and a != 1)
                    if p == 1:
                        from_inner(a, 0, q).wait_recv()
                        acc = final(a, 0, q, [part(iin[a].at[0], a, q)], acc)
                    return acc

                acc = lax.fori_loop(0, CHUNKS, both, acc)
        fbuf[...] = acc[:8] + acc[8:]
        drain(OUTR, osr)

    @pl.when(jnp.logical_not(is_end))
    def _():
        def inward(p, a, q):
            from_end(a, p, q).wait_recv()
            i = p * 12 + a * CHUNKS + q
            send(a, 3 - p, q, [part(ein[a].at[p], a, q)], OUTR, osr, part(iin[a].at[p], a, q), ir.at[i], inner, p == 0 and a != 1)

        def outward(a, q):
            from_inner(a, 0, q).wait_recv()
            send(a, 0, q, [part(iin[a].at[0], a, q)], OUTL, osl, part(iin[a].at[0], a, q), ir.at[a * CHUNKS + q], outer, a != 1)

        for copy in lend(0):
            copy.start()
        for a in range(4):
            if a > 0:
                give_terms((0, 2, 1)[a - 1])

            def both(q, a=a):
                more_terms(0, a, q)
                if a < 3:
                    inward(0, a, q)
                if a > 0:
                    outward(a - 1, q)

            loop(both)
        for copy in lend(1):
            copy.start()
        for a in range(3):
            for copy in moments(a):
                copy.start()
        for a in range(3):
            loop(functools.partial(inward, 1, a))
        acc = zero
        for a in range(3):

            def last(q, acc, a=a):
                from_inner(a, 1, q).wait_recv()
                from_end(a, 2, q).wait_recv()
                acc = final(a, 1, q, [part(ein[a].at[2], a, q), part(iin[a].at[1], a, q)], acc)
                if a == LENT:
                    lend_sum(q).start()
                return acc

            acc = lax.fori_loop(0, CHUNKS, last, acc)
        fbuf[...] = acc[:8] + acc[8:]
        drain(OUTR, osr)
        drain(OUTL, osl)

    nb[me] = fbuf[...]
    sums = [remote(nb.at[me], nb.at[me], ns.at[d], nr.at[d], (me + d) % GROUP) for d in range(1, GROUP)]
    for copy in sums:
        copy.start()
    for copy in sums:
        copy.wait()

    squares = nb[0]
    for d in range(1, GROUP):
        squares = squares + nb[d]
    squares = jnp.sum(jnp.sum(squares, axis=0, keepdims=True), axis=1, keepdims=True)
    factor = jnp.minimum(1.0, 0.5 * lax.rsqrt(squares / count + 1e-30))
    fbuf[...] = jnp.broadcast_to(factor, fbuf.shape)

    def give(a, q, J, src, to_inner, to_outer):
        c = a * CHUNKS + q
        dst = full(t[a], a, J, k, q)
        remote(src, dst, sp.at[J * 12 + c], pr.at[J * 12 + c], partner).start()
        if to_inner is not None:
            remote(src, dst, si.at[to_inner[0] * 12 + c], ar.at[to_inner[1] * 12 + c], inner).start()
        if to_outer is not None:
            remote(src, dst, so.at[to_outer * 12 + c], ar.at[to_outer * 12 + c], outer).start()

    def stepped(a, q, J, mv, at_row):
        c, slot = kind[a], q % 2
        l, s = at_layer(q)
        start = (2 * chip(J) + k) * rows_of[a] + s * half_of[a]

        def row(r, _):
            here = pl.ds(pl.multiple_of(r * ROWS, ROWS), ROWS)
            there = pl.ds(pl.multiple_of(start + r * ROWS, ROWS), ROWS)
            those = pl.ds(pl.multiple_of(at_row + r * ROWS, ROWS), ROWS)
            (m_in, v_in), layer = mv, l if len(mv[0].shape) == 3 else None
            at = (those, slice(None)) if layer is None else (layer, those, slice(None))
            one = t[a][l, there, :].astype(F32) * fbuf[0:1, 0:1]
            m1 = 0.9 * m_in[at] + 0.1 * one
            v1 = 0.95 * v_in[at] + 0.05 * one * one
            if layer is not None:
                m_in[at] = m1
                v_in[at] = v1
            old = wb[c][slot, here, :].astype(F32)
            t[a][l, there, :] = (old - 0.02 * (m1 * lax.rsqrt(v1 + 1e-8) + 0.1 * old)).astype(BF16)
            return 0

        lax.fori_loop(0, half_of[a] // ROWS, row, 0)

    for n, a in enumerate(ORDER):
        if a == LENT:

            @pl.when(jnp.logical_not(is_end))
            def _():
                for q in range(CHUNKS):
                    lend_sum(q).wait_send()

        for copy in moments(a):
            copy.wait()

        def update(q, n=n, a=a):
            old_weight(a, q).wait()

            @pl.when(q < CHUNKS - 1)
            def _():
                old_weight(a, q + 1).start()

            if n < 2:

                @pl.when(q == CHUNKS - 1)
                def _():
                    old_weight(ORDER[n + 1], q * 0).start()

            stepped(a, q, own_J, (nm[a], nv[a]), at_layer(q)[1] * half_of[a])
            src = full(t[a], a, own_J, k, q)

            @pl.when(is_end)
            def _():
                give(a, q, 0, src, (0, 2), None)

            @pl.when(jnp.logical_not(is_end))
            def _():
                give(a, q, 1, src, (0, 0), None if a == LENT else 0)

        loop(update)

    @pl.when(is_end)
    def _():
        def lent(q):
            a = LENT
            lend_sum(q).wait_recv()

            @pl.when(q % HALVES == 0)
            def _():
                for copy in lend(q // HALVES):
                    copy.wait_recv()

            copies = (
                pltpu.make_async_copy(part(xm, a, q), lm, up.at[2]),
                pltpu.make_async_copy(part(xv, a, q), lv, up.at[3]),
                old_weight(a, q, 1),
            )
            for copy in copies:
                copy.start()
            for copy in copies:
                copy.wait()
            stepped(a, q, 1, (lm, lv), 0)
            give(a, q, 1, full(t[a], a, 1, k, q), None, None)

        loop(lent)

    def arrived(a, q, J, slot):
        here = full(t[a], a, J, k, q)
        remote(here, here, sp.at[0], ar.at[slot * 12 + a * CHUNKS + q], inner).wait_recv()

    @pl.when(is_end)
    def _():
        for slot in range(3):
            for a in ORDER:
                if slot == 0 and a == LENT:
                    continue

                def on(q, a=a, slot=slot):
                    arrived(a, q, slot + 1, slot)
                    give(a, q, slot + 1, full(t[a], a, slot + 1, k, q), None, None)

                loop(on)

    @pl.when(jnp.logical_not(is_end))
    def _():
        for a in ORDER:

            def on(q, a=a):
                arrived(a, q, 2, 0)
                give(a, q, 2, full(t[a], a, 2, k, q), None, 1)
                arrived(a, q, 0, 2)
                give(a, q, 0, full(t[a], a, 0, k, q), (1, 1), None)

            loop(on)
        for a in ORDER:

            def on(q, a=a):
                arrived(a, q, 3, 1)
                give(a, q, 3, full(t[a], a, 3, k, q), None, 2)

            loop(on)

    for a in range(3):

        def rest(q, a=a):
            c = a * CHUNKS + q
            for J in range(4):
                mine, theirs = full(t[a], a, J, k, q), full(t[a], a, J, 1 - k, q)
                remote(mine, mine, sp.at[J * 12 + c], pr.at[J * 12 + c], partner).wait_send()
                remote(theirs, theirs, sp.at[J * 12 + c], pr.at[J * 12 + c], partner).wait_recv()
            here = full(t[a], a, own_J, k, q)
            remote(here, here, si.at[c], ar.at[c], inner).wait_send()

            @pl.when(jnp.logical_not(is_end))
            def _():
                remote(here, here, si.at[12 + c], ar.at[c], inner).wait_send()
                for n in range(1 if a == LENT else 0, 3):
                    remote(here, here, so.at[n * 12 + c], ar.at[c], outer).wait_send()

        loop(rest)
        for J in range(4):
            for l in range(2):
                swap(J, a, l).wait_send()

    @pl.when(jnp.logical_not(is_end))
    def _():
        for l in range(2):
            for copy in lend(l):
                copy.wait_send()


def finish(*refs):
    n = (len(refs) - 1) // 2
    copies = [
        pltpu.make_async_copy(refs[i].at[l], refs[n + i].at[l], refs[-1].at[i, l]) for i in range(n) for l in range(refs[i].shape[0])
    ]
    for copy in copies:
        copy.start()
    for copy in copies:
        copy.wait()


def solution(mesh):
    def step(*arrays):
        terms, weights, m, v = (arrays[i : i + 3] for i in (0, 3, 6, 9))
        blocks = [one.shape for one in m]
        count = GROUP * sum(one.size for one in m)
        pair = (blocks[0], blocks[2])
        chunk = [(one[1] // HALVES, one[2]) for one in pair]
        results = [(one.shape, BF16) for one in weights] + [(one, F32) for one in blocks] * 2
        dma, in_vmem, in_hbm = pltpu.SemaphoreType.DMA, pl.BlockSpec(memory_space=pltpu.VMEM), pl.BlockSpec(memory_space=pltpu.HBM)
        slots = [pltpu.HBM((n, *one), BF16) for n in (4, 3, 2) for one in blocks] + [pltpu.HBM(blocks[LENT], F32)] * 2
        out = pl.pallas_call(
            functools.partial(kernel, count),
            out_shape=[pltpu.VMEM(*one) for one in results] + slots,
            in_specs=[in_hbm] * 12,
            out_specs=[in_vmem] * 9 + [in_hbm] * 11,
            scratch_shapes=[pltpu.VMEM((2, *one), BF16) for one in chunk]
            + [pltpu.VMEM(chunk[0], F32)] * 2
            + [pltpu.VMEM((GROUP, 8, 128), F32), pltpu.VMEM((8, 128), F32)]
            + [dma((n,)) for n in (4, 4, 4, 24, 24, 36, 24, 4, 8, 8, 36, 48, 36, 24, 48, 4, 4, 4, 4, 6)],
            compiler_params=pltpu.CompilerParams(collective_id=0, has_side_effects=True, vmem_limit_bytes=LIMIT),
            name="step",
        )(*(pltpu.with_memory_space_constraint(one, pltpu.HBM) for one in arrays))[:9]
        return pl.pallas_call(
            finish,
            out_shape=[jax.ShapeDtypeStruct(*one) for one in results],
            in_specs=[in_vmem] * 9,
            out_specs=[pl.BlockSpec(memory_space=pl.ANY)] * 9,
            scratch_shapes=[dma((9, 2))],
            compiler_params=pltpu.CompilerParams(vmem_limit_bytes=LIMIT),
            name="finish",
        )(*(pltpu.with_memory_space_constraint(one, pltpu.VMEM) for one in out))

    all_of, cut = P(None, None, None), P(None, "dp", None)
    return jax.shard_map(
        step,
        mesh=mesh,
        in_specs=(P(("rep", "dp"), None, None, None),) * 3 + (all_of,) * 3 + (cut,) * 6,
        out_specs=(P("rep", None, None),) * 3 + (P("rep", "dp", None),) * 6,
        check_vma=False,
    )
```

```python
import functools

import jax
import jax.numpy as jnp
from jax import lax
from jax.experimental import pallas as pl
from jax.experimental.pallas import tpu as pltpu
from jax.sharding import PartitionSpec as P

F32, BF16 = jnp.float32, jnp.bfloat16
HALVES = 2
CHUNKS = 4
GROUP = 8
OUTR, OUTL = 3, 5
LAG = 2
LIMIT = 5 * 2**20
ROWS = 16


def kernel(count, *refs):
    g, w, m, v = refs[0:3], refs[3:6], refs[6:9], refs[9:12]
    t, nm, nv = refs[12:15], refs[15:18], refs[18:21]
    x, ein, iin = refs[21:24], refs[24:27], refs[27:30]
    wb, nb, fbuf = refs[30:32], refs[32], refs[33]
    (ld, osr, osl, xs, xr, er, ir, up, ns, nr, ar, pr, so, si, sp, gs, gr, mo) = refs[34:]

    me = lax.axis_index("dp")
    z, k = me // 2, me % 2
    h = z // 2
    is_end = (z % 3) == 0
    inner, outer = 2 * (z + 1 - 2 * h) + k, 2 * (z - 1 + 2 * h) + k
    partner = 2 * z + 1 - k
    kind = (0, 0, 1)
    rows_of = [r.shape[1] for r in m]
    half_of = [r // HALVES for r in rows_of]

    def chip(J):
        return J + h * (3 - 2 * J)

    def at_layer(q):
        return q // HALVES, q % HALVES

    def full(ref, a, J, parity, q):
        l, s = at_layer(q)
        start = pl.multiple_of((2 * chip(J) + parity) * rows_of[a] + s * half_of[a], 16)
        return ref.at[l, pl.ds(start, half_of[a]), :]

    def part(ref, a, q):
        l, s = at_layer(q)
        return ref.at[l, pl.ds(pl.multiple_of(s * half_of[a], 16), half_of[a]), :]

    def slot_start(c, i):
        rows, half = rows_of[c + 1], half_of[c + 1]
        return pl.multiple_of(((2 * z + k) * rows + 3 * rows + i * half) % (GROUP * rows), 16)

    def staged(c, i):
        return t[c + 1].at[0, pl.ds(slot_start(c, i), half_of[c + 1]), :]

    def staged_rows(c, i, r):
        return 0, pl.ds(pl.multiple_of(slot_start(c, i) + r * ROWS, ROWS), ROWS), slice(None)

    def remote(src, dst, send, recv, to):
        return pltpu.make_async_remote_copy(src, dst, send, recv, device_id={"dp": to}, device_id_type=pl.DeviceIdType.MESH)

    barrier = pltpu.get_barrier_semaphore()
    for d in range(1, GROUP):
        pl.semaphore_signal(barrier, inc=1, device_id={"dp": (me + d) % GROUP}, device_id_type=pl.DeviceIdType.MESH)
    pl.semaphore_wait(barrier, GROUP - 1)

    def swap(J, a, l):
        start = pl.multiple_of((2 * chip(J) + 1 - k) * rows_of[a], 16)
        return remote(g[a].at[0, l, pl.ds(start, rows_of[a]), :], x[a].at[J, l], xs.at[J * 6 + a * 2 + l], xr.at[J * 6 + a * 2 + l], partner)

    def give_terms(J, weights=(0, 1, 2)):
        for a in weights:
            for l in range(2):
                swap(J, a, l).start()

    order = [(p, a) for p in range(2) for a in range(3)]

    def give_next(n):
        if n < len(order):
            p, a = order[n]
            give_terms(3 - p, (a,))
            give_terms(p, (a,))

    give_terms(3, (0,))

    own_J = jnp.where(is_end, 0, 1)

    def old_weight(a, q, J=own_J):
        return pltpu.make_async_copy(full(w[a], a, J, k, q), wb[kind[a]].at[q % 2], up.at[q % 2])

    old_weight(0, 0).start()

    def moments(a):
        return pltpu.make_async_copy(m[a], nm[a], mo.at[a]), pltpu.make_async_copy(v[a], nv[a], mo.at[3 + a])

    def load(a, J, q, more):
        l, s = at_layer(q)

        @pl.when(s == 0)
        def _():
            remote(x[a].at[J, l], x[a].at[J, l], xs.at[J * 6 + a * 2 + l], xr.at[J * 6 + a * 2 + l], partner).wait_recv()

        sources = [full(g[a].at[0], a, J, k, q), part(x[a].at[J], a, q), *more]
        copies = [pltpu.make_async_copy(src, staged(kind[a], i), ld.at[i]) for i, src in enumerate(sources)]
        for copy in copies:
            copy.start()
        for copy in copies:
            copy.wait()
        return len(copies)

    def total(a, n, r):
        so_far = t[kind[a] + 1][staged_rows(kind[a], 0, r)].astype(F32)
        for i in range(1, n):
            so_far = so_far + t[kind[a] + 1][staged_rows(kind[a], i, r)].astype(F32)
        return so_far.astype(BF16)

    def send(a, J, q, more, out, sem, dst, recv, to, first):
        c, slot = kind[a], q % 2
        copy = remote(staged(c, out + slot), dst, sem.at[c * 2 + slot], recv, to)
        n = load(a, J, q, more)
        if first:

            @pl.when(q >= 2)
            def _():
                copy.wait_send()
        else:
            copy.wait_send()

        def row(r, _):
            t[c + 1][staged_rows(c, out + slot, r)] = total(a, n, r)
            return 0

        lax.fori_loop(0, half_of[a] // ROWS, row, 0)
        copy.start()

    def final(a, J, into, q, more, acc):
        l, s = at_layer(q)
        n = load(a, J, q, more)

        def row(r, acc):
            one = total(a, n, r)
            t[a][l, pl.ds(pl.multiple_of((2 * chip(into) + k) * rows_of[a] + s * half_of[a] + r * ROWS, ROWS), ROWS), :] = one
            one = one.astype(F32)
            one = one * one
            for i in range(one.shape[1] // 128):
                acc = acc + one[:, i * 128 : (i + 1) * 128]
            return acc

        return lax.fori_loop(0, half_of[a] // ROWS, row, acc)

    def more_terms(n, q):
        if n == 0:

            @pl.when(q == 1)
            def _():
                give_terms(0, (0,))
                give_next(1)

    def sum_for_mid(a, q, to):
        return remote(full(t[a], a, 3, k, q), full(t[a], a, 1, k, q), gs.at[a * CHUNKS + q], gr.at[a * CHUNKS + q], to)

    def from_end(a, p, q):
        i = p * 12 + a * CHUNKS + q
        return remote(part(ein[a].at[p], a, q), part(ein[a].at[p], a, q), osr.at[0], er.at[i], outer)

    def from_inner(a, p, q):
        i = p * 12 + a * CHUNKS + q
        return remote(part(iin[a].at[p], a, q), part(iin[a].at[p], a, q), osr.at[0], ir.at[i], inner)

    def loop(body):
        lax.fori_loop(0, CHUNKS, lambda q, _: (body(q), 0)[1], 0)

    zero = jnp.zeros((ROWS, 128), F32)

    def drain(out, sem):
        for a in (1, 2):
            for slot in range(2):
                one, on = staged(kind[a], out + slot), sem.at[kind[a] * 2 + slot]
                remote(one, one, on, on, inner).wait_send()

    @pl.when(is_end)
    def _():
        acc = zero
        for n in range(len(order) + 1):
            if n > 0:
                give_next(n + 1)
            if n == 3:
                for a in range(3):
                    for copy in moments(a):
                        copy.start()

            def both(q, acc, n=n):
                more_terms(n, q)
                if n < len(order):
                    p, a = order[n]
                    i = p * 12 + a * CHUNKS + q
                    send(a, 3 - p, q, [], OUTR, osr, part(ein[a].at[p], a, q), er.at[i], inner, p == 0 and a != 1)
                if n > 0:
                    p, a = order[n - 1]
                    from_inner(a, p, q).wait_recv()
                    acc = final(a, p, (0, 3)[p], q, [part(iin[a].at[p], a, q)], acc)
                if n == len(order):
                    @pl.when(q > 0)
                    def _():
                        sum_for_mid(0, q - 1, inner).wait_send()

                    @pl.when(q < CHUNKS - 1)
                    def _():
                        sum_for_mid(0, q, inner).start()

                return acc

            acc = lax.fori_loop(0, CHUNKS, both, acc)
        fbuf[...] = acc[:8] + acc[8:]
        drain(OUTR, osr)

    @pl.when(jnp.logical_not(is_end))
    def _():
        def inward(p, a, q):
            from_end(a, p, q).wait_recv()
            i = p * 12 + a * CHUNKS + q
            send(a, 3 - p, q, [part(ein[a].at[p], a, q)], OUTR, osr, part(iin[a].at[p], a, q), ir.at[i], inner, p == 0 and a != 1)

        def outward(p, a, q):
            from_inner(a, p, q).wait_recv()
            i = p * 12 + a * CHUNKS + q
            send(a, p, q, [part(iin[a].at[p], a, q)], OUTL, osl, part(iin[a].at[p], a, q), ir.at[i], outer, p == 0 and a != 1)

        for n in range(len(order) + 1):
            if n > 0:
                give_next(n + 1)
            if n == 3:
                for a in range(3):
                    for copy in moments(a):
                        copy.start()

            def early(q, n=n):
                more_terms(n, q)
                if n < len(order):
                    inward(*order[n], q)
                if n > 0:
                    outward(*order[n - 1], q + CHUNKS - LAG)

            def late(q, n=n):
                inward(*order[n], q)
                outward(*order[n], q - LAG)

            lax.fori_loop(0, LAG, lambda q, _: (early(q), 0)[1], 0)
            if n < len(order):
                lax.fori_loop(LAG, CHUNKS, lambda q, _: (late(q), 0)[1], 0)
        fbuf[...] = zero[:8]
        drain(OUTR, osr)
        drain(OUTL, osl)

    nb[me] = fbuf[...]
    sums = [remote(nb.at[me], nb.at[me], ns.at[d], nr.at[d], (me + d) % GROUP) for d in range(1, GROUP)]
    for copy in sums:
        copy.start()

    @pl.when(is_end)
    def _():
        sum_for_mid(0, CHUNKS - 1, inner).start()
        for a in (1, 2):
            loop(lambda q, a=a: sum_for_mid(a, q, inner).start())

    for copy in sums:
        copy.wait()

    squares = nb[0]
    for d in range(1, GROUP):
        squares = squares + nb[d]
    squares = jnp.sum(jnp.sum(squares, axis=0, keepdims=True), axis=1, keepdims=True)
    factor = jnp.minimum(1.0, 0.5 * lax.rsqrt(squares / count + 1e-30))
    fbuf[...] = jnp.broadcast_to(factor, fbuf.shape)

    def give(a, q, J, src, to_inner, to_outer):
        c = a * CHUNKS + q
        dst = full(t[a], a, J, k, q)
        remote(src, dst, sp.at[J * 12 + c], pr.at[J * 12 + c], partner).start()
        if to_inner is not None:
            remote(src, dst, si.at[to_inner[0] * 12 + c], ar.at[to_inner[1] * 12 + c], inner).start()
        if to_outer is not None:
            remote(src, dst, so.at[to_outer * 12 + c], ar.at[to_outer * 12 + c], outer).start()

    def stepped(a, q):
        c, slot = kind[a], q % 2
        l, s = at_layer(q)
        start = (2 * z + k) * rows_of[a] + s * half_of[a]

        def row(r, _):
            here = pl.ds(pl.multiple_of(r * ROWS, ROWS), ROWS)
            there = pl.ds(pl.multiple_of(start + r * ROWS, ROWS), ROWS)
            those = pl.ds(pl.multiple_of(s * half_of[a] + r * ROWS, ROWS), ROWS)
            one = t[a][l, there, :].astype(F32) * fbuf[0:1, 0:1]
            m1 = 0.9 * nm[a][l, those, :] + 0.1 * one
            v1 = 0.95 * nv[a][l, those, :] + 0.05 * one * one
            nm[a][l, those, :] = m1
            nv[a][l, those, :] = v1
            old = wb[c][slot, here, :].astype(F32)
            t[a][l, there, :] = (old - 0.02 * (m1 * lax.rsqrt(v1 + 1e-8) + 0.1 * old)).astype(BF16)
            return 0

        lax.fori_loop(0, half_of[a] // ROWS, row, 0)

    for a in range(3):
        for copy in moments(a):
            copy.wait()

        def update(q, a=a):
            old_weight(a, q).wait()

            @pl.when(q < CHUNKS - 1)
            def _():
                old_weight(a, q + 1).start()

            if a < 2:

                @pl.when(q == CHUNKS - 1)
                def _():
                    old_weight(a + 1, q * 0).start()

            @pl.when(jnp.logical_not(is_end))
            def _():
                sum_for_mid(a, q, outer).wait_recv()

            stepped(a, q)
            src = full(t[a], a, own_J, k, q)

            @pl.when(is_end)
            def _():
                give(a, q, 0, src, None, None)

            @pl.when(jnp.logical_not(is_end))
            def _():
                give(a, q, 1, src, (0, 0), 0)

        loop(update)

    @pl.when(is_end)
    def _():
        sum_for_mid(0, CHUNKS - 1, inner).wait_send()
        for a in (1, 2):
            loop(lambda q, a=a: sum_for_mid(a, q, inner).wait_send())
        for a in range(3):

            def pass_on(q, a=a):
                c, src = a * CHUNKS + q, full(t[a], a, 0, k, q)
                remote(src, src, si.at[c], ar.at[24 + c], inner).start()

            loop(pass_on)

    def arrived(a, q, J, slot):
        here = full(t[a], a, J, k, q)
        remote(here, here, sp.at[0], ar.at[slot * 12 + a * CHUNKS + q], inner).wait_recv()

    @pl.when(is_end)
    def _():
        for slot in range(3):
            for a in range(3):

                def on(q, a=a, slot=slot):
                    arrived(a, q, slot + 1, slot)
                    give(a, q, slot + 1, full(t[a], a, slot + 1, k, q), None, None)

                loop(on)

    @pl.when(jnp.logical_not(is_end))
    def _():
        for a in range(3):

            def on(q, a=a):
                arrived(a, q, 2, 0)
                give(a, q, 2, full(t[a], a, 2, k, q), None, 1)
                arrived(a, q, 0, 2)
                give(a, q, 0, full(t[a], a, 0, k, q), (1, 1), None)

            loop(on)
        for a in range(3):

            def on(q, a=a):
                arrived(a, q, 3, 1)
                give(a, q, 3, full(t[a], a, 3, k, q), None, 2)

            loop(on)

    for a in range(3):

        def rest(q, a=a):
            c = a * CHUNKS + q
            for J in range(4):
                mine, theirs = full(t[a], a, J, k, q), full(t[a], a, J, 1 - k, q)
                remote(mine, mine, sp.at[J * 12 + c], pr.at[J * 12 + c], partner).wait_send()
                remote(theirs, theirs, sp.at[J * 12 + c], pr.at[J * 12 + c], partner).wait_recv()
            here = full(t[a], a, own_J, k, q)
            remote(here, here, si.at[c], ar.at[c], inner).wait_send()

            @pl.when(jnp.logical_not(is_end))
            def _():
                remote(here, here, si.at[12 + c], ar.at[c], inner).wait_send()
                for n in range(3):
                    remote(here, here, so.at[n * 12 + c], ar.at[c], outer).wait_send()

        loop(rest)
        for J in range(4):
            for l in range(2):
                swap(J, a, l).wait_send()


def finish(*refs):
    n = (len(refs) - 1) // 2
    copies = [
        pltpu.make_async_copy(refs[i].at[l], refs[n + i].at[l], refs[-1].at[i, l]) for i in range(n) for l in range(refs[i].shape[0])
    ]
    for copy in copies:
        copy.start()
    for copy in copies:
        copy.wait()


def solution(mesh):
    def step(*arrays):
        terms, weights, m, v = (arrays[i : i + 3] for i in (0, 3, 6, 9))
        blocks = [one.shape for one in m]
        count = GROUP * sum(one.size for one in m)
        pair = (blocks[0], blocks[2])
        chunk = [(one[1] // HALVES, one[2]) for one in pair]
        results = [(one.shape, BF16) for one in weights] + [(one, F32) for one in blocks] * 2
        dma, in_vmem, in_hbm = pltpu.SemaphoreType.DMA, pl.BlockSpec(memory_space=pltpu.VMEM), pl.BlockSpec(memory_space=pltpu.HBM)
        slots = [pltpu.HBM((n, *one), BF16) for n in (4, 2, 2) for one in blocks]
        out = pl.pallas_call(
            functools.partial(kernel, count),
            out_shape=[pltpu.VMEM(*one) for one in results] + slots,
            in_specs=[in_hbm] * 12,
            out_specs=[in_vmem] * 9 + [in_hbm] * 9,
            scratch_shapes=[pltpu.VMEM((2, *one), BF16) for one in chunk]
            + [pltpu.VMEM((GROUP, 8, 128), F32), pltpu.VMEM((8, 128), F32)]
            + [dma((n,)) for n in (4, 4, 4, 24, 24, 24, 24, 2, 8, 8, 36, 48, 36, 24, 48, 12, 12, 6)],
            compiler_params=pltpu.CompilerParams(collective_id=0, has_side_effects=True, vmem_limit_bytes=LIMIT),
            name="step",
        )(*(pltpu.with_memory_space_constraint(one, pltpu.HBM) for one in arrays))[:9]
        return pl.pallas_call(
            finish,
            out_shape=[jax.ShapeDtypeStruct(*one) for one in results],
            in_specs=[in_vmem] * 9,
            out_specs=[pl.BlockSpec(memory_space=pl.ANY)] * 9,
            scratch_shapes=[dma((9, 2))],
            compiler_params=pltpu.CompilerParams(vmem_limit_bytes=LIMIT),
            name="finish",
        )(*(pltpu.with_memory_space_constraint(one, pltpu.VMEM) for one in out))

    all_of, cut = P(None, None, None), P(None, "dp", None)
    return jax.shard_map(
        step,
        mesh=mesh,
        in_specs=(P(("rep", "dp"), None, None, None),) * 3 + (all_of,) * 3 + (cut,) * 6,
        out_specs=(P("rep", None, None),) * 3 + (P("rep", "dp", None),) * 6,
        check_vma=False,
    )
```

```python
import functools

import jax
import jax.numpy as jnp
from jax import lax
from jax.experimental import pallas as pl
from jax.experimental.pallas import tpu as pltpu
from jax.sharding import PartitionSpec as P

F32, BF16 = jnp.float32, jnp.bfloat16
CUTS = (4, 4, 2)
CHUNKS = (8, 8, 4)
BASE = (0, 8, 16)
ALL = 20
TURNS = 4
ORDER = (0, 2, 1)
GROUP = 8
OUTR, OUTL = 3, 5
LAG = 1
LIMIT = 5 * 2**20
ROWS = 16


def kernel(count, *refs):
    g, w, m, v = refs[0:3], refs[3:6], refs[6:9], refs[9:12]
    t, nm, nv = refs[12:15], refs[15:18], refs[18:21]
    x, ein, iin = refs[21:24], refs[24:27], refs[27:30]
    wb, nb, fbuf = refs[30:32], refs[32], refs[33]
    (ld, osr, osl, xs, xr, er, ir, up, ns, nr, ar, pr, so, si, sp, gs, gr, mo) = refs[34:]

    me = lax.axis_index("dp")
    z, k = me // 2, me % 2
    h = z // 2
    is_end = (z % 3) == 0
    inner, outer = 2 * (z + 1 - 2 * h) + k, 2 * (z - 1 + 2 * h) + k
    partner = 2 * z + 1 - k
    kind = (0, 0, 1)
    rows_of = [r.shape[1] for r in m]
    half_of = [r // cuts for r, cuts in zip(rows_of, CUTS, strict=True)]
    per = [n // TURNS for n in CHUNKS]

    def chip(J):
        return J + h * (3 - 2 * J)

    def at_layer(a, q):
        return q // CUTS[a], q % CUTS[a]

    def full(ref, a, J, parity, q):
        l, s = at_layer(a, q)
        start = pl.multiple_of((2 * chip(J) + parity) * rows_of[a] + s * half_of[a], 16)
        return ref.at[l, pl.ds(start, half_of[a]), :]

    def part(ref, a, q):
        l, s = at_layer(a, q)
        return ref.at[l, pl.ds(pl.multiple_of(s * half_of[a], 16), half_of[a]), :]

    def slot_start(c, i):
        rows, half = rows_of[c + 1], half_of[c + 1]
        return pl.multiple_of(((2 * z + k) * rows + 3 * rows + i * half) % (GROUP * rows), 16)

    def staged(c, i):
        return t[c + 1].at[0, pl.ds(slot_start(c, i), half_of[c + 1]), :]

    def staged_rows(c, i, r):
        return 0, pl.ds(pl.multiple_of(slot_start(c, i) + r * ROWS, ROWS), ROWS), slice(None)

    def remote(src, dst, send, recv, to):
        return pltpu.make_async_remote_copy(src, dst, send, recv, device_id={"dp": to}, device_id_type=pl.DeviceIdType.MESH)

    barrier = pltpu.get_barrier_semaphore()
    for d in range(1, GROUP):
        pl.semaphore_signal(barrier, inc=1, device_id={"dp": (me + d) % GROUP}, device_id_type=pl.DeviceIdType.MESH)
    pl.semaphore_wait(barrier, GROUP - 1)

    def swap(J, a, l):
        start = pl.multiple_of((2 * chip(J) + 1 - k) * rows_of[a], 16)
        return remote(g[a].at[0, l, pl.ds(start, rows_of[a]), :], x[a].at[J, l], xs.at[J * 6 + a * 2 + l], xr.at[J * 6 + a * 2 + l], partner)

    def give_terms(J, weights=(0, 1, 2)):
        for a in weights:
            for l in range(2):
                swap(J, a, l).start()

    order = [(p, a) for p in range(2) for a in ORDER]

    def give_next(n):
        if n < len(order):
            p, a = order[n]
            give_terms(3 - p, (a,))
            give_terms(p, (a,))

    give_terms(3, ORDER[:1])

    own_J = jnp.where(is_end, 0, 1)

    def old_weight(a, q, J=own_J):
        return pltpu.make_async_copy(full(w[a], a, J, k, q), wb[kind[a]].at[q % 2], up.at[q % 2])

    old_weight(ORDER[0], 0).start()

    def moments(a):
        return pltpu.make_async_copy(m[a], nm[a], mo.at[a]), pltpu.make_async_copy(v[a], nv[a], mo.at[3 + a])

    def load(a, J, q, more):
        l, s = at_layer(a, q)

        @pl.when(s == 0)
        def _():
            remote(x[a].at[J, l], x[a].at[J, l], xs.at[J * 6 + a * 2 + l], xr.at[J * 6 + a * 2 + l], partner).wait_recv()

        sources = [full(g[a].at[0], a, J, k, q), part(x[a].at[J], a, q), *more]
        copies = [pltpu.make_async_copy(src, staged(kind[a], i), ld.at[i]) for i, src in enumerate(sources)]
        for copy in copies:
            copy.start()
        for copy in copies:
            copy.wait()
        return len(copies)

    def total(a, n, r):
        so_far = t[kind[a] + 1][staged_rows(kind[a], 0, r)].astype(F32)
        for i in range(1, n):
            so_far = so_far + t[kind[a] + 1][staged_rows(kind[a], i, r)].astype(F32)
        return so_far.astype(BF16)

    def send(a, J, q, more, out, sem, dst, recv, to, first):
        c, slot = kind[a], q % 2
        copy = remote(staged(c, out + slot), dst, sem.at[c * 2 + slot], recv, to)
        n = load(a, J, q, more)
        if first:

            @pl.when(q >= 2)
            def _():
                copy.wait_send()
        else:
            copy.wait_send()

        def row(r, _):
            t[c + 1][staged_rows(c, out + slot, r)] = total(a, n, r)
            return 0

        lax.fori_loop(0, half_of[a] // ROWS, row, 0)
        copy.start()

    def final(a, J, into, q, more, acc):
        l, s = at_layer(a, q)
        n = load(a, J, q, more)

        def row(r, acc):
            one = total(a, n, r)
            t[a][l, pl.ds(pl.multiple_of((2 * chip(into) + k) * rows_of[a] + s * half_of[a] + r * ROWS, ROWS), ROWS), :] = one
            one = one.astype(F32)
            one = one * one
            for i in range(one.shape[1] // 128):
                acc = acc + one[:, i * 128 : (i + 1) * 128]
            return acc

        return lax.fori_loop(0, half_of[a] // ROWS, row, acc)

    def more_terms(n, q):
        if n == 0:

            @pl.when(q == 1)
            def _():
                give_terms(0, ORDER[:1])
                give_next(1)

    def sum_for_mid(a, q, to):
        return remote(full(t[a], a, 3, k, q), full(t[a], a, 1, k, q), gs.at[BASE[a] + q], gr.at[BASE[a] + q], to)

    def from_end(a, p, q):
        i = p * ALL + BASE[a] + q
        return remote(part(ein[a].at[p], a, q), part(ein[a].at[p], a, q), osr.at[0], er.at[i], outer)

    def from_inner(a, p, q):
        i = p * ALL + BASE[a] + q
        return remote(part(iin[a].at[p], a, q), part(iin[a].at[p], a, q), osr.at[0], ir.at[i], inner)

    def loop(a, body):
        lax.fori_loop(0, CHUNKS[a], lambda q, _: (body(q), 0)[1], 0)

    def turn(a, q):
        return [(a, q * per[a] + i) for i in range(per[a])]

    zero = jnp.zeros((ROWS, 128), F32)

    def drain(out, sem):
        for a in (1, 2):
            for slot in range(2):
                one, on = staged(kind[a], out + slot), sem.at[kind[a] * 2 + slot]
                remote(one, one, on, on, inner).wait_send()

    @pl.when(is_end)
    def _():
        acc = zero
        for n in range(len(order) + 1):
            if n > 0:
                give_next(n + 1)
            if n == 3:
                for a in range(3):
                    for copy in moments(a):
                        copy.start()

            def both(q, acc, n=n):
                more_terms(n, q)
                if n < len(order):
                    p, a = order[n]
                    for a, c in turn(a, q):
                        i = p * ALL + BASE[a] + c
                        send(a, 3 - p, c, [], OUTR, osr, part(ein[a].at[p], a, c), er.at[i], inner, p == 0 and a != 1)
                if n > 0:
                    p, a = order[n - 1]
                    for a, c in turn(a, q):
                        from_inner(a, p, c).wait_recv()
                        acc = final(a, p, (0, 3)[p], c, [part(iin[a].at[p], a, c)], acc)
                if n == len(order):
                    @pl.when(q > 0)
                    def _():
                        for a, c in turn(ORDER[0], q - 1):
                            sum_for_mid(a, c, inner).wait_send()

                    @pl.when(q < TURNS - 1)
                    def _():
                        for a, c in turn(ORDER[0], q):
                            sum_for_mid(a, c, inner).start()

                return acc

            acc = lax.fori_loop(0, TURNS, both, acc)
        fbuf[...] = acc[:8] + acc[8:]
        drain(OUTR, osr)

    @pl.when(jnp.logical_not(is_end))
    def _():
        def inward(p, a, q):
            from_end(a, p, q).wait_recv()
            i = p * ALL + BASE[a] + q
            send(a, 3 - p, q, [part(ein[a].at[p], a, q)], OUTR, osr, part(iin[a].at[p], a, q), ir.at[i], inner, p == 0 and a != 1)

        def outward(p, a, q):
            from_inner(a, p, q).wait_recv()
            i = p * ALL + BASE[a] + q
            send(a, p, q, [part(iin[a].at[p], a, q)], OUTL, osl, part(iin[a].at[p], a, q), ir.at[i], outer, p == 0 and a != 1)

        for n in range(len(order) + 1):
            if n > 0:
                give_next(n + 1)
            if n == 3:
                for a in range(3):
                    for copy in moments(a):
                        copy.start()

            def some(ins, outs):
                for i in range(max(len(ins), len(outs))):
                    if i < len(ins):
                        inward(*ins[i])
                    if i < len(outs):
                        outward(*outs[i])

            def chunks(n, q):
                if not 0 <= n < len(order):
                    return []
                return [(order[n][0], a, c) for a, c in turn(order[n][1], q)]

            def early(q, n=n):
                more_terms(n, q)
                some(chunks(n, q), chunks(n - 1, q + TURNS - LAG))

            def late(q, n=n):
                more_terms(n, q)
                some(chunks(n, q), chunks(n, q - LAG))

            lax.fori_loop(0, LAG, lambda q, _: (early(q), 0)[1], 0)
            if n < len(order):
                lax.fori_loop(LAG, TURNS, lambda q, _: (late(q), 0)[1], 0)
        fbuf[...] = zero[:8]
        drain(OUTR, osr)
        drain(OUTL, osl)

    nb[me] = fbuf[...]
    sums = [remote(nb.at[me], nb.at[me], ns.at[d], nr.at[d], (me + d) % GROUP) for d in range(1, GROUP)]
    for copy in sums:
        copy.start()

    @pl.when(is_end)
    def _():
        for a, q in turn(ORDER[0], TURNS - 1):
            sum_for_mid(a, q, inner).start()
        for a in ORDER[1:]:
            loop(a, lambda q, a=a: sum_for_mid(a, q, inner).start())

    for copy in sums:
        copy.wait()

    squares = nb[0]
    for d in range(1, GROUP):
        squares = squares + nb[d]
    squares = jnp.sum(jnp.sum(squares, axis=0, keepdims=True), axis=1, keepdims=True)
    factor = jnp.minimum(1.0, 0.5 * lax.rsqrt(squares / count + 1e-30))
    fbuf[...] = jnp.broadcast_to(factor, fbuf.shape)

    def give(a, q, J, src, to_inner, to_outer):
        c = BASE[a] + q
        dst = full(t[a], a, J, k, q)
        remote(src, dst, sp.at[J * ALL + c], pr.at[J * ALL + c], partner).start()
        if to_inner is not None:
            remote(src, dst, si.at[to_inner[0] * ALL + c], ar.at[to_inner[1] * ALL + c], inner).start()
        if to_outer is not None:
            remote(src, dst, so.at[to_outer * ALL + c], ar.at[to_outer * ALL + c], outer).start()

    def stepped(a, q):
        c, slot = kind[a], q % 2
        l, s = at_layer(a, q)
        start = (2 * z + k) * rows_of[a] + s * half_of[a]

        def row(r, _):
            here = pl.ds(pl.multiple_of(r * ROWS, ROWS), ROWS)
            there = pl.ds(pl.multiple_of(start + r * ROWS, ROWS), ROWS)
            those = pl.ds(pl.multiple_of(s * half_of[a] + r * ROWS, ROWS), ROWS)
            one = t[a][l, there, :].astype(F32) * fbuf[0:1, 0:1]
            m1 = 0.9 * nm[a][l, those, :] + 0.1 * one
            v1 = 0.95 * nv[a][l, those, :] + 0.05 * one * one
            nm[a][l, those, :] = m1
            nv[a][l, those, :] = v1
            old = wb[c][slot, here, :].astype(F32)
            t[a][l, there, :] = (old - 0.02 * (m1 * lax.rsqrt(v1 + 1e-8) + 0.1 * old)).astype(BF16)
            return 0

        lax.fori_loop(0, half_of[a] // ROWS, row, 0)

    for n, a in enumerate(ORDER):
        for copy in moments(a):
            copy.wait()

        def update(q, n=n, a=a):
            old_weight(a, q).wait()

            @pl.when(q < CHUNKS[a] - 1)
            def _():
                old_weight(a, q + 1).start()

            if n < 2:

                @pl.when(q == CHUNKS[a] - 1)
                def _():
                    old_weight(ORDER[n + 1], q * 0).start()

            @pl.when(jnp.logical_not(is_end))
            def _():
                sum_for_mid(a, q, outer).wait_recv()

            stepped(a, q)
            src = full(t[a], a, own_J, k, q)

            @pl.when(is_end)
            def _():
                give(a, q, 0, src, None, None)

            @pl.when(jnp.logical_not(is_end))
            def _():
                give(a, q, 1, src, (0, 0), 0)

        loop(a, update)

    @pl.when(is_end)
    def _():
        for a, q in turn(ORDER[0], TURNS - 1):
            sum_for_mid(a, q, inner).wait_send()
        for a in ORDER[1:]:
            loop(a, lambda q, a=a: sum_for_mid(a, q, inner).wait_send())
        for a in ORDER:

            def pass_on(q, a=a):
                c, src = BASE[a] + q, full(t[a], a, 0, k, q)
                remote(src, src, si.at[c], ar.at[2 * ALL + c], inner).start()

            loop(a, pass_on)

    def arrived(a, q, J, slot):
        here = full(t[a], a, J, k, q)
        remote(here, here, sp.at[0], ar.at[slot * ALL + BASE[a] + q], inner).wait_recv()

    @pl.when(is_end)
    def _():
        for slot in range(3):
            for a in ORDER:

                def on(q, a=a, slot=slot):
                    arrived(a, q, slot + 1, slot)
                    give(a, q, slot + 1, full(t[a], a, slot + 1, k, q), None, None)

                loop(a, on)

    @pl.when(jnp.logical_not(is_end))
    def _():
        for a in ORDER:

            def on(q, a=a):
                arrived(a, q, 2, 0)
                give(a, q, 2, full(t[a], a, 2, k, q), None, 1)
                arrived(a, q, 0, 2)
                give(a, q, 0, full(t[a], a, 0, k, q), (1, 1), None)

            loop(a, on)
        for a in ORDER:

            def on(q, a=a):
                arrived(a, q, 3, 1)
                give(a, q, 3, full(t[a], a, 3, k, q), None, 2)

            loop(a, on)

    for a in range(3):

        def rest(q, a=a):
            c = BASE[a] + q
            for J in range(4):
                mine, theirs = full(t[a], a, J, k, q), full(t[a], a, J, 1 - k, q)
                remote(mine, mine, sp.at[J * ALL + c], pr.at[J * ALL + c], partner).wait_send()
                remote(theirs, theirs, sp.at[J * ALL + c], pr.at[J * ALL + c], partner).wait_recv()
            here = full(t[a], a, own_J, k, q)
            remote(here, here, si.at[c], ar.at[c], inner).wait_send()

            @pl.when(jnp.logical_not(is_end))
            def _():
                remote(here, here, si.at[ALL + c], ar.at[c], inner).wait_send()
                for n in range(3):
                    remote(here, here, so.at[n * ALL + c], ar.at[c], outer).wait_send()

        loop(a, rest)
        for J in range(4):
            for l in range(2):
                swap(J, a, l).wait_send()


def finish(*refs):
    n = (len(refs) - 1) // 2
    copies = [
        pltpu.make_async_copy(refs[i].at[l], refs[n + i].at[l], refs[-1].at[i, l]) for i in range(n) for l in range(refs[i].shape[0])
    ]
    for copy in copies:
        copy.start()
    for copy in copies:
        copy.wait()


def solution(mesh):
    def step(*arrays):
        terms, weights, m, v = (arrays[i : i + 3] for i in (0, 3, 6, 9))
        blocks = [one.shape for one in m]
        count = GROUP * sum(one.size for one in m)
        pair = (blocks[0], blocks[2])
        chunk = [(one[1] // cuts, one[2]) for one, cuts in zip(pair, CUTS[1:], strict=True)]
        results = [(one.shape, BF16) for one in weights] + [(one, F32) for one in blocks] * 2
        dma, in_vmem, in_hbm = pltpu.SemaphoreType.DMA, pl.BlockSpec(memory_space=pltpu.VMEM), pl.BlockSpec(memory_space=pltpu.HBM)
        slots = [pltpu.HBM((n, *one), BF16) for n in (4, 2, 2) for one in blocks]
        out = pl.pallas_call(
            functools.partial(kernel, count),
            out_shape=[pltpu.VMEM(*one) for one in results] + slots,
            in_specs=[in_hbm] * 12,
            out_specs=[in_vmem] * 9 + [in_hbm] * 9,
            scratch_shapes=[pltpu.VMEM((2, *one), BF16) for one in chunk]
            + [pltpu.VMEM((GROUP, 8, 128), F32), pltpu.VMEM((8, 128), F32)]
            + [dma((n,)) for n in (4, 4, 4, 24, 24, 2 * ALL, 2 * ALL, 2, 8, 8, 3 * ALL, 4 * ALL, 3 * ALL, 2 * ALL, 4 * ALL, ALL, ALL, 6)],
            compiler_params=pltpu.CompilerParams(collective_id=0, has_side_effects=True, vmem_limit_bytes=LIMIT),
            name="step",
        )(*(pltpu.with_memory_space_constraint(one, pltpu.HBM) for one in arrays))[:9]
        return pl.pallas_call(
            finish,
            out_shape=[jax.ShapeDtypeStruct(*one) for one in results],
            in_specs=[in_vmem] * 9,
            out_specs=[pl.BlockSpec(memory_space=pl.ANY)] * 9,
            scratch_shapes=[dma((9, 2))],
            compiler_params=pltpu.CompilerParams(vmem_limit_bytes=LIMIT),
            name="finish",
        )(*(pltpu.with_memory_space_constraint(one, pltpu.VMEM) for one in out))

    all_of, cut = P(None, None, None), P(None, "dp", None)
    return jax.shard_map(
        step,
        mesh=mesh,
        in_specs=(P(("rep", "dp"), None, None, None),) * 3 + (all_of,) * 3 + (cut,) * 6,
        out_specs=(P("rep", None, None),) * 3 + (P("rep", "dp", None),) * 6,
        check_vma=False,
    )
```

```python
import functools

import jax
import jax.numpy as jnp
from jax import lax
from jax.experimental import pallas as pl
from jax.experimental.pallas import tpu as pltpu
from jax.sharding import PartitionSpec as P

F32, BF16 = jnp.float32, jnp.bfloat16
CUTS = (4, 4, 2)
CHUNKS = (8, 8, 4)
BASE = (0, 8, 16)
ALL = 20
TURNS = 4
ORDER = (0, 2, 1)
KEPT = 2
GROUP = 8
OUTR, OUTL = 4, 6
LAG = 1
LIMIT = 5 * 2**20
ROWS = 16


def kernel(count, *refs):
    g, w, m, v = refs[0:3], refs[3:6], refs[6:9], refs[9:12]
    t, nm, nv = refs[12:15], refs[15:18], refs[18:21]
    x, ein, iin = refs[21:24], refs[24:27], refs[27:30]
    wb, nb, fbuf = refs[30:32], refs[32], refs[33]
    (ld, osr, osl, xs, xr, er, ir, up, ns, nr, ar, pr, so, si, sp, gs, gr, mo) = refs[34:]

    me = lax.axis_index("dp")
    z, k = me // 2, me % 2
    h = z // 2
    is_end = (z % 3) == 0
    inner, outer = 2 * (z + 1 - 2 * h) + k, 2 * (z - 1 + 2 * h) + k
    partner = 2 * z + 1 - k
    kind = (0, 0, 1)
    rows_of = [r.shape[1] for r in m]
    half_of = [r // cuts for r, cuts in zip(rows_of, CUTS, strict=True)]
    per = [n // TURNS for n in CHUNKS]

    def chip(J):
        return J + h * (3 - 2 * J)

    def at_layer(a, q):
        return q // CUTS[a], q % CUTS[a]

    def full(ref, a, J, parity, q):
        l, s = at_layer(a, q)
        start = pl.multiple_of((2 * chip(J) + parity) * rows_of[a] + s * half_of[a], 16)
        return ref.at[l, pl.ds(start, half_of[a]), :]

    def part(ref, a, q):
        l, s = at_layer(a, q)
        return ref.at[l, pl.ds(pl.multiple_of(s * half_of[a], 16), half_of[a]), :]

    def slot_start(c, i):
        rows, half = rows_of[c + 1], half_of[c + 1]
        return pl.multiple_of(((2 * z + k) * rows + 3 * rows + i * half) % (GROUP * rows), 16)

    def staged(c, i):
        return t[c + 1].at[0, pl.ds(slot_start(c, i), half_of[c + 1]), :]

    def staged_rows(c, i, r):
        return 0, pl.ds(pl.multiple_of(slot_start(c, i) + r * ROWS, ROWS), ROWS), slice(None)

    def remote(src, dst, send, recv, to):
        return pltpu.make_async_remote_copy(src, dst, send, recv, device_id={"dp": to}, device_id_type=pl.DeviceIdType.MESH)

    barrier = pltpu.get_barrier_semaphore()
    for d in range(1, GROUP):
        pl.semaphore_signal(barrier, inc=1, device_id={"dp": (me + d) % GROUP}, device_id_type=pl.DeviceIdType.MESH)
    pl.semaphore_wait(barrier, GROUP - 1)

    def swap(J, a, l):
        start = pl.multiple_of((2 * chip(J) + 1 - k) * rows_of[a], 16)
        return remote(g[a].at[0, l, pl.ds(start, rows_of[a]), :], x[a].at[J, l], xs.at[J * 6 + a * 2 + l], xr.at[J * 6 + a * 2 + l], partner)

    def give_terms(J, weights=(0, 1, 2)):
        for a in weights:
            for l in range(2):
                swap(J, a, l).start()

    order = [(p, a) for p in range(2) for a in ORDER]

    def give_next(n):
        if n < len(order):
            p, a = order[n]
            give_terms(3 - p, (a,))
            give_terms(p, (a,))

    give_terms(3, ORDER[:1])

    own_J = jnp.where(is_end, 0, 1)

    def old_weight(a, q, J=own_J):
        return pltpu.make_async_copy(full(w[a], a, J, k, q), wb[kind[a]].at[q % 2], up.at[q % 2])

    old_weight(ORDER[0], 0).start()

    def moments(a):
        return pltpu.make_async_copy(m[a], nm[a], mo.at[a]), pltpu.make_async_copy(v[a], nv[a], mo.at[3 + a])

    def load(a, J, q, more, first_layer=False):
        l, s = at_layer(a, q)

        @pl.when(q == 0 if first_layer else s == 0)
        def _():
            remote(x[a].at[J, l], x[a].at[J, l], xs.at[J * 6 + a * 2 + l], xr.at[J * 6 + a * 2 + l], partner).wait_recv()

        sources = [full(g[a].at[0], a, J, k, q), part(x[a].at[J], a, q), *more]
        copies = [pltpu.make_async_copy(src, staged(kind[a], i), ld.at[i]) for i, src in enumerate(sources)]
        for copy in copies:
            copy.start()
        for copy in copies:
            copy.wait()
        return len(copies)

    def total(a, n, r):
        so_far = t[kind[a] + 1][staged_rows(kind[a], 0, r)].astype(F32)
        for i in range(1, n):
            so_far = so_far + t[kind[a] + 1][staged_rows(kind[a], i, r)].astype(F32)
        return so_far.astype(BF16)

    def send(a, J, q, more, out, sem, dst, recv, to, first):
        c, slot = kind[a], q % 2
        copy = remote(staged(c, out + slot), dst, sem.at[c * 2 + slot], recv, to)
        n = load(a, J, q, more)
        if first:

            @pl.when(q >= 2)
            def _():
                copy.wait_send()
        else:
            copy.wait_send()

        def row(r, _):
            t[c + 1][staged_rows(c, out + slot, r)] = total(a, n, r)
            return 0

        lax.fori_loop(0, half_of[a] // ROWS, row, 0)
        copy.start()

    def final(a, J, into, q, more, acc, first_layer=False):
        l, s = at_layer(a, q)
        n = load(a, J, q, more, first_layer)

        def row(r, acc):
            one = total(a, n, r)
            t[a][l, pl.ds(pl.multiple_of((2 * chip(into) + k) * rows_of[a] + s * half_of[a] + r * ROWS, ROWS), ROWS), :] = one
            one = one.astype(F32)
            one = one * one
            for i in range(one.shape[1] // 128):
                acc = acc + one[:, i * 128 : (i + 1) * 128]
            return acc

        return lax.fori_loop(0, half_of[a] // ROWS, row, acc)

    def more_terms(n, q):
        if n == 0:

            @pl.when(q == 1)
            def _():
                give_terms(0, ORDER[:1])
                give_next(1)

    def sum_for_mid(a, q, to):
        return remote(full(t[a], a, 3, k, q), full(t[a], a, 1, k, q), gs.at[BASE[a] + q], gr.at[BASE[a] + q], to)

    def from_end(a, p, q):
        i = p * ALL + BASE[a] + q
        return remote(part(ein[a].at[p], a, q), part(ein[a].at[p], a, q), osr.at[0], er.at[i], outer)

    def from_inner(a, p, q):
        i = p * ALL + BASE[a] + q
        return remote(part(iin[a].at[p], a, q), part(iin[a].at[p], a, q), osr.at[0], ir.at[i], inner)

    def given(a):
        return CHUNKS[a] - KEPT if a == ORDER[-1] else CHUNKS[a]

    def loop(a, body):
        lax.fori_loop(0, CHUNKS[a], lambda q, _: (body(q), 0)[1], 0)

    def turn(a, q):
        return [(a, q * per[a] + i) for i in range(per[a])]

    zero = jnp.zeros((ROWS, 128), F32)

    def drain(out, sem):
        for a in (1, 2):
            for slot in range(2):
                one, on = staged(kind[a], out + slot), sem.at[kind[a] * 2 + slot]
                remote(one, one, on, on, inner).wait_send()

    @pl.when(is_end)
    def _():
        acc = zero
        for n in range(len(order) + 1):
            if n > 0:
                give_next(n + 1)
            if n == 3:
                for a in range(3):
                    for copy in moments(a):
                        copy.start()

            if n == len(order):
                a = ORDER[-1]
                l = CHUNKS[a] // CUTS[a] - 1
                swap(1, a, l).wait_recv()
                for c in range(CHUNKS[a] - KEPT, CHUNKS[a]):
                    send(a, 1, c, [], OUTR, osr, part(ein[a].at[2], a, c), er.at[2 * ALL + BASE[a] + c], inner, False)

            def both(q, acc, n=n):
                more_terms(n, q)
                if n < len(order):
                    p, a = order[n]
                    for a, c in turn(a, q):
                        i = p * ALL + BASE[a] + c
                        send(a, 3 - p, c, [], OUTR, osr, part(ein[a].at[p], a, c), er.at[i], inner, p == 0 and a != 1)
                if n > 0:
                    p, a = order[n - 1]
                    for a, c in turn(a, q):
                        from_inner(a, p, c).wait_recv()
                        acc = final(a, p, (0, 3)[p], c, [part(iin[a].at[p], a, c)], acc, n == len(order))
                return acc

            acc = lax.fori_loop(0, TURNS if n < len(order) else TURNS - 1, both, acc)
        fbuf[...] = acc[:8] + acc[8:]
        drain(OUTR, osr)

    @pl.when(jnp.logical_not(is_end))
    def _():
        def inward(p, a, q):
            from_end(a, p, q).wait_recv()
            i = p * ALL + BASE[a] + q
            send(a, 3 - p, q, [part(ein[a].at[p], a, q)], OUTR, osr, part(iin[a].at[p], a, q), ir.at[i], inner, p == 0 and a != 1)

        def outward(p, a, q):
            from_inner(a, p, q).wait_recv()
            i = p * ALL + BASE[a] + q
            send(a, p, q, [part(iin[a].at[p], a, q)], OUTL, osl, part(iin[a].at[p], a, q), ir.at[i], outer, p == 0 and a != 1)

        for n in range(len(order) + 1):
            if n > 0:
                give_next(n + 1)
            if n == 3:
                for a in range(3):
                    for copy in moments(a):
                        copy.start()

            def some(ins, outs):
                for i in range(max(len(ins), len(outs))):
                    if i < len(ins):
                        inward(*ins[i])
                    if i < len(outs):
                        outward(*outs[i])

            def chunks(n, q):
                if not 0 <= n < len(order):
                    return []
                return [(order[n][0], a, c) for a, c in turn(order[n][1], q)]

            def early(q, n=n):
                more_terms(n, q)
                some(chunks(n, q), chunks(n - 1, q + TURNS - LAG))

            def late(q, n=n):
                more_terms(n, q)
                some(chunks(n, q), chunks(n, q - LAG))

            if n < len(order):
                lax.fori_loop(0, LAG, lambda q, _: (early(q), 0)[1], 0)
                lax.fori_loop(LAG, TURNS, lambda q, _: (late(q), 0)[1], 0)
        acc, a = zero, ORDER[-1]
        for c in range(CHUNKS[a] - KEPT, CHUNKS[a]):
            from_inner(a, 1, c).wait_recv()
            from_end(a, 2, c).wait_recv()
            acc = final(a, 1, 1, c, [part(iin[a].at[1], a, c), part(ein[a].at[2], a, c)], acc)
        fbuf[...] = acc[:8] + acc[8:]
        drain(OUTR, osr)
        drain(OUTL, osl)

    nb[me] = fbuf[...]
    sums = [remote(nb.at[me], nb.at[me], ns.at[d], nr.at[d], (me + d) % GROUP) for d in range(1, GROUP)]
    for copy in sums:
        copy.start()


    @pl.when(is_end)
    def _():
        for a in ORDER:
            lax.fori_loop(0, given(a), lambda q, _, a=a: (sum_for_mid(a, q, inner).start(), 0)[1], 0)

    for copy in sums:
        copy.wait()

    squares = nb[0]
    for d in range(1, GROUP):
        squares = squares + nb[d]
    squares = jnp.sum(jnp.sum(squares, axis=0, keepdims=True), axis=1, keepdims=True)
    factor = jnp.minimum(1.0, 0.5 * lax.rsqrt(squares / count + 1e-30))
    fbuf[...] = jnp.broadcast_to(factor, fbuf.shape)

    def give(a, q, J, src, to_inner, to_outer):
        c = BASE[a] + q
        dst = full(t[a], a, J, k, q)
        remote(src, dst, sp.at[J * ALL + c], pr.at[J * ALL + c], partner).start()
        if to_inner is not None:
            remote(src, dst, si.at[to_inner[0] * ALL + c], ar.at[to_inner[1] * ALL + c], inner).start()
        if to_outer is not None:
            remote(src, dst, so.at[to_outer * ALL + c], ar.at[to_outer * ALL + c], outer).start()

    def stepped(a, q):
        c, slot = kind[a], q % 2
        l, s = at_layer(a, q)
        start = (2 * z + k) * rows_of[a] + s * half_of[a]

        def row(r, _):
            here = pl.ds(pl.multiple_of(r * ROWS, ROWS), ROWS)
            there = pl.ds(pl.multiple_of(start + r * ROWS, ROWS), ROWS)
            those = pl.ds(pl.multiple_of(s * half_of[a] + r * ROWS, ROWS), ROWS)
            one = t[a][l, there, :].astype(F32) * fbuf[0:1, 0:1]
            m1 = 0.9 * nm[a][l, those, :] + 0.1 * one
            v1 = 0.95 * nv[a][l, those, :] + 0.05 * one * one
            nm[a][l, those, :] = m1
            nv[a][l, those, :] = v1
            old = wb[c][slot, here, :].astype(F32)
            t[a][l, there, :] = (old - 0.02 * (m1 * lax.rsqrt(v1 + 1e-8) + 0.1 * old)).astype(BF16)
            return 0

        lax.fori_loop(0, half_of[a] // ROWS, row, 0)

    for n, a in enumerate(ORDER):
        for copy in moments(a):
            copy.wait()

        def update(q, n=n, a=a):
            old_weight(a, q).wait()

            @pl.when(q < CHUNKS[a] - 1)
            def _():
                old_weight(a, q + 1).start()

            if n < 2:

                @pl.when(q == CHUNKS[a] - 1)
                def _():
                    old_weight(ORDER[n + 1], q * 0).start()

            @pl.when(jnp.logical_and(jnp.logical_not(is_end), q < given(a)))
            def _():
                sum_for_mid(a, q, outer).wait_recv()

            stepped(a, q)
            src = full(t[a], a, own_J, k, q)

            @pl.when(is_end)
            def _():
                give(a, q, 0, src, None, None)

            @pl.when(jnp.logical_not(is_end))
            def _():
                give(a, q, 1, src, (0, 0), 0)

        loop(a, update)

    @pl.when(is_end)
    def _():
        for a in ORDER:
            lax.fori_loop(0, given(a), lambda q, _, a=a: (sum_for_mid(a, q, inner).wait_send(), 0)[1], 0)
        for a in ORDER:

            def pass_on(q, a=a):
                c, src = BASE[a] + q, full(t[a], a, 0, k, q)
                remote(src, src, si.at[c], ar.at[2 * ALL + c], inner).start()

            loop(a, pass_on)

    def arrived(a, q, J, slot):
        here = full(t[a], a, J, k, q)
        remote(here, here, sp.at[0], ar.at[slot * ALL + BASE[a] + q], inner).wait_recv()

    @pl.when(is_end)
    def _():
        for slot in range(3):
            for a in ORDER:

                def on(q, a=a, slot=slot):
                    arrived(a, q, slot + 1, slot)
                    give(a, q, slot + 1, full(t[a], a, slot + 1, k, q), None, None)

                loop(a, on)

    @pl.when(jnp.logical_not(is_end))
    def _():
        for a in ORDER:

            def on(q, a=a):
                arrived(a, q, 2, 0)
                give(a, q, 2, full(t[a], a, 2, k, q), None, 1)
                arrived(a, q, 0, 2)
                give(a, q, 0, full(t[a], a, 0, k, q), (1, 1), None)

            loop(a, on)
        for a in ORDER:

            def on(q, a=a):
                arrived(a, q, 3, 1)
                give(a, q, 3, full(t[a], a, 3, k, q), None, 2)

            loop(a, on)

    for a in range(3):

        def rest(q, a=a):
            c = BASE[a] + q
            for J in range(4):
                mine, theirs = full(t[a], a, J, k, q), full(t[a], a, J, 1 - k, q)
                remote(mine, mine, sp.at[J * ALL + c], pr.at[J * ALL + c], partner).wait_send()
                remote(theirs, theirs, sp.at[J * ALL + c], pr.at[J * ALL + c], partner).wait_recv()
            here = full(t[a], a, own_J, k, q)
            remote(here, here, si.at[c], ar.at[c], inner).wait_send()

            @pl.when(jnp.logical_not(is_end))
            def _():
                remote(here, here, si.at[ALL + c], ar.at[c], inner).wait_send()
                for n in range(3):
                    remote(here, here, so.at[n * ALL + c], ar.at[c], outer).wait_send()

        loop(a, rest)
        for J in range(4):
            for l in range(2):
                swap(J, a, l).wait_send()


def finish(*refs):
    n = (len(refs) - 1) // 2
    copies = [
        pltpu.make_async_copy(refs[i].at[l], refs[n + i].at[l], refs[-1].at[i, l]) for i in range(n) for l in range(refs[i].shape[0])
    ]
    for copy in copies:
        copy.start()
    for copy in copies:
        copy.wait()


def solution(mesh):
    def step(*arrays):
        terms, weights, m, v = (arrays[i : i + 3] for i in (0, 3, 6, 9))
        blocks = [one.shape for one in m]
        count = GROUP * sum(one.size for one in m)
        pair = (blocks[0], blocks[2])
        chunk = [(one[1] // cuts, one[2]) for one, cuts in zip(pair, CUTS[1:], strict=True)]
        results = [(one.shape, BF16) for one in weights] + [(one, F32) for one in blocks] * 2
        dma, in_vmem, in_hbm = pltpu.SemaphoreType.DMA, pl.BlockSpec(memory_space=pltpu.VMEM), pl.BlockSpec(memory_space=pltpu.HBM)
        slots = [pltpu.HBM((n, *one), BF16) for n in (4, 3, 2) for one in blocks]
        out = pl.pallas_call(
            functools.partial(kernel, count),
            out_shape=[pltpu.VMEM(*one) for one in results] + slots,
            in_specs=[in_hbm] * 12,
            out_specs=[in_vmem] * 9 + [in_hbm] * 9,
            scratch_shapes=[pltpu.VMEM((2, *one), BF16) for one in chunk]
            + [pltpu.VMEM((GROUP, 8, 128), F32), pltpu.VMEM((8, 128), F32)]
            + [dma((n,)) for n in (4, 4, 4, 24, 24, 3 * ALL, 2 * ALL, 2, 8, 8, 3 * ALL, 4 * ALL, 3 * ALL, 2 * ALL, 4 * ALL, ALL, ALL, 6)],
            compiler_params=pltpu.CompilerParams(collective_id=0, has_side_effects=True, vmem_limit_bytes=LIMIT),
            name="step",
        )(*(pltpu.with_memory_space_constraint(one, pltpu.HBM) for one in arrays))[:9]
        return pl.pallas_call(
            finish,
            out_shape=[jax.ShapeDtypeStruct(*one) for one in results],
            in_specs=[in_vmem] * 9,
            out_specs=[pl.BlockSpec(memory_space=pl.ANY)] * 9,
            scratch_shapes=[dma((9, 2))],
            compiler_params=pltpu.CompilerParams(vmem_limit_bytes=LIMIT),
            name="finish",
        )(*(pltpu.with_memory_space_constraint(one, pltpu.VMEM) for one in out))

    all_of, cut = P(None, None, None), P(None, "dp", None)
    return jax.shard_map(
        step,
        mesh=mesh,
        in_specs=(P(("rep", "dp"), None, None, None),) * 3 + (all_of,) * 3 + (cut,) * 6,
        out_specs=(P("rep", None, None),) * 3 + (P("rep", "dp", None),) * 6,
        check_vma=False,
    )
```
